32 devices in a mesh: section: 4 (over z), dp: 4 (over y, x), mp: 2 (over core).
Axes of the slice: x: 2, y: 2, z: 4, core: 2. Of those that a mesh axis runs over, the one named last changes fastest.
Arguments:
- fwd_in: bfloat16 [4, 2048, 1024], P('section', ('dp', 'mp')), may hold values from -6 to 6
- stash: bfloat16 [4, 2048, 1024], P('section', ('dp', 'mp')), may hold values from -6 to 6
- cot: bfloat16 [4, 2048, 1024], P('section', ('dp', 'mp')), may hold values from -8 to 8
- w_in: bfloat16 [4, 2048, 1024], P('section', 'mp'), may hold values from -0.1875 to 0.1875
- w_out: bfloat16 [4, 2048, 1024], P('section', 'mp'), may hold values from -0.125 to 0.125
- gain: float32 [4, 1024], P('section'), may hold values from 0.1 to 1.9
Outputs:
- passed_fwd: bfloat16 [4, 2048, 1024], P('section', ('dp', 'mp'))
- passed_grad: bfloat16 [4, 2048, 1024], P('section', ('dp', 'mp'))
- grad_w_in: bfloat16 [4, 2048, 1024], P('section', 'mp', 'dp')
- grad_w_out: bfloat16 [4, 2048, 1024], P('section', 'mp', 'dp')
The draws below stay inside these ranges and needn't reach their ends.
All inputs are finite; a program needn't handle non-finite values.
Results may differ from the reference program's by a relative error of at most 0.015.
Values may be sent and summed in bfloat16 or wider, within the bound.
A program may use at most 64 MiB of HBM per device.

```python
import jax
import jax.numpy as jnp
from jax import lax

D = 1024
HID = 2048
TOK = 512
HID_DEV = 1024
TOKENS = 2048
SECTIONS = 4
N_DP = 4
N_MP = 2


def raised(array, rng, source, target, blocks, factor):
    def block_of(axis_at):
        return (jnp.arange(array.shape[axis_at]) // (array.shape[axis_at] // blocks)).reshape((-1,) + (1,) * (array.ndim - 1 - axis_at))

    one_side = jax.random.permutation(rng, blocks)[block_of(target)]
    other_side = (block_of(target) + blocks // 2) % blocks
    return jnp.where((block_of(source) == one_side) | (block_of(source) == other_side), factor * array, array)


def steps_of(own_key, shape, split, least, high):
    level, own = 1.0, jax.random.fold_in(own_key, 6)
    for position, blocks in split:
        steps = jnp.exp(jax.random.uniform(jax.random.fold_in(own, position), (blocks,), jnp.float32, least / len(split), high / len(split)))
        level = level * jnp.repeat(steps, shape[position] // blocks).reshape([-1 if axis == position else 1 for axis in range(len(shape))])
    return level


def gaussian(key, shape, width, reach, pieces=(), dtype=jnp.bfloat16):
    result = width * jax.random.normal(key, shape, jnp.float32)
    if pieces:
        result = result * steps_of(key, shape, pieces, -0.22, 0.18)
    return jnp.clip(result, -reach, reach).astype(dtype)


def heavy_noise(rng, dims, deviation, most, pieces, heavy, held_as=jnp.bfloat16):
    entries = deviation * jax.random.normal(rng, dims, jnp.float32)
    if pieces:
        entries = entries * steps_of(rng, dims, pieces, -0.22, 0.18)
    return jnp.clip(raised(entries, jax.random.fold_in(rng, 3), *heavy), -most, most).astype(held_as)


def setup_inputs(seed: int = 0) -> dict:
    streams_of = jax.random.split(jax.random.key(seed), 7)
    fwd_in = gaussian(streams_of[0], (SECTIONS, TOKENS, D), 1.0, 6.0, ((0, 4), (1, 8)))
    stash = gaussian(streams_of[1], (SECTIONS, TOKENS, D), 1.0, 6.0, ((0, 4), (1, 8)))
    cot = heavy_noise(streams_of[2], (SECTIONS, TOKENS, D), 1.0, 8.0, ((0, 4), (1, 8)), (1, 2, 8, 2.0))
    w_in = gaussian(streams_of[3], (SECTIONS, HID, D), D ** -0.5, 0.1875, ((0, 4), (1, 2)))
    w_out = gaussian(streams_of[4], (SECTIONS, HID, D), HID ** -0.5, 0.125, ((0, 4), (1, 2)))
    gain = jnp.clip(1.0 + 0.18 * jax.random.normal(streams_of[5], (SECTIONS, D), jnp.float32), 0.1, 1.9)
    return {"fwd_in": fwd_in, "stash": stash, "cot": cot, "w_in": w_in, "w_out": w_out, "gain": gain}


norm_eps = 1e-05
gelu_coef = 0.7978845608

def gelu_value(v):
    inner = jnp.tanh(gelu_coef * (v + 0.044715 * v * v * v))
    return 0.5 * v * (1.0 + inner)

def gelu_slope(v):
    inner = jnp.tanh(gelu_coef * (v + 0.044715 * v * v * v))
    return 0.5 * (1.0 + inner) + 0.5 * v * (1.0 - inner * inner) * gelu_coef * (1.0 + 0.134145 * v * v)

def prepare(x, w_in, gain):
    xf = x.astype(jnp.float32)
    scale = lax.rsqrt(lax.optimization_barrier(jnp.mean(xf * xf, axis=-1, keepdims=True)) + norm_eps)
    normed = (xf * scale * gain[None, :]).astype(jnp.bfloat16)
    pre = lax.dot_general(normed, w_in, (((1,), (1,)), ((), ())), preferred_element_type=jnp.float32)
    act = gelu_value(pre).astype(jnp.bfloat16)
    return (xf, scale, normed, pre, act)

def group_sum(left, right):
    rows = left.shape[0]
    lhs = left.reshape(rows, N_MP, HID_DEV).astype(jnp.float32)
    rhs = right.reshape(N_MP, HID_DEV, right.shape[1]).astype(jnp.float32)
    parts = jnp.einsum('tgh,ghd->gtd', lhs, rhs).astype(jnp.bfloat16)
    parts = lax.optimization_barrier(parts)
    return lax.optimization_barrier(jnp.sum(parts.astype(jnp.float32), axis=0))

def replica_sum(left, right):
    lhs = left.reshape(N_DP, TOK, left.shape[1]).astype(jnp.float32)
    rhs = right.reshape(N_DP, TOK, right.shape[1]).astype(jnp.float32)
    parts = jnp.einsum('rth,rtd->rhd', lhs, rhs).astype(jnp.bfloat16)
    parts = lax.optimization_barrier(parts)
    return lax.optimization_barrier(jnp.sum(parts.astype(jnp.float32), axis=0)).astype(jnp.bfloat16)

def reference(fwd_in, stash, cot, w_in, w_out, gain):
    outs = []
    grads = []
    g_ins = []
    g_outs = []
    for section in range(SECTIONS):
        xf, scale, normed, pre, act = prepare(fwd_in[section], w_in[section], gain[section])
        outs.append((xf + group_sum(act, w_out[section])).astype(jnp.bfloat16))
        sf, sscale, snormed, spre, sact = prepare(stash[section], w_in[section], gain[section])
        cot_rows = cot[section]
        d_act = lax.dot_general(cot_rows, w_out[section], (((1,), (1,)), ((), ())), preferred_element_type=jnp.float32)
        d_pre = (d_act * gelu_slope(spre)).astype(jnp.bfloat16)
        d_norm = group_sum(d_pre, w_in[section])
        push = d_norm * gain[section][None, :]
        mixed = lax.optimization_barrier(jnp.mean(sf * push, axis=-1, keepdims=True))
        dx = cot_rows.astype(jnp.float32) + sscale * push - sf * sscale * sscale * sscale * mixed
        grads.append(dx.astype(jnp.bfloat16))
        g_outs.append(replica_sum(sact, cot_rows))
        g_ins.append(replica_sum(d_pre, snormed))
    passed_fwd = jnp.roll(jnp.stack(outs), 1, axis=0)
    passed_grad = jnp.roll(jnp.stack(grads), -1, axis=0)
    return (passed_fwd, passed_grad, jnp.stack(g_ins), jnp.stack(g_outs))
```

```python
import jax
import jax.numpy as jnp
from jax import lax
from jax.experimental import pallas as pl
from jax.experimental.pallas import tpu as pltpu
from jax.sharding import PartitionSpec as P

norm_eps = 1e-05
gelu_coef = 0.7978845608


def shifted(x, axis, by):
    length = lax.axis_size(axis)
    return lax.ppermute(x, axis, [(i, (i + by) % length) for i in range(length)])


def gelu_value(v):
    inner = jnp.tanh(gelu_coef * (v + 0.044715 * v * v * v))
    return 0.5 * v * (1.0 + inner)


def gelu_slope(v):
    inner = jnp.tanh(gelu_coef * (v + 0.044715 * v * v * v))
    return 0.5 * (1.0 + inner) + 0.5 * v * (1.0 - inner * inner) * gelu_coef * (
        1.0 + 0.134145 * v * v
    )


def prepare(x, w_first, gain_row):
    xf = x.astype(jnp.float32)
    scale = lax.rsqrt(jnp.mean(xf * xf, axis=-1, keepdims=True) + norm_eps)
    normed = (xf * scale * gain_row[None, :]).astype(jnp.bfloat16)
    pre = lax.dot_general(
        normed, w_first, (((1,), (1,)), ((), ())), preferred_element_type=jnp.float32
    )
    act = gelu_value(pre).astype(jnp.bfloat16)
    return (scale, normed, pre, act)


def on_device(fwd_in, stash, cot, w_in, w_out, gain):
    x_fwd = fwd_in[0]
    x_bwd = stash[0]
    cot_local = cot[0]
    w_first = w_in[0]
    w_second = w_out[0]
    gain_row = gain[0]
    local_rows = x_fwd.shape[0]
    scale, normed, pre, act = prepare(
        lax.all_gather(x_fwd, "mp", axis=0, tiled=True), w_first, gain_row
    )
    terms = jnp.dot(act, w_second, preferred_element_type=jnp.float32)
    branch = lax.psum_scatter(
        terms.astype(jnp.bfloat16), "mp", scatter_dimension=0, tiled=True
    ).astype(jnp.float32)
    out = (x_fwd.astype(jnp.float32) + branch).astype(jnp.bfloat16)
    passed_fwd = shifted(out, "section", 1)
    rows_x, rows_cot = (
        lax.all_gather(x_bwd, "mp", axis=0, tiled=True),
        lax.all_gather(cot_local, "mp", axis=0, tiled=True),
    )
    scale, normed, pre, act = prepare(rows_x, w_first, gain_row)
    d_act = lax.dot_general(
        rows_cot, w_second, (((1,), (1,)), ((), ())), preferred_element_type=jnp.float32
    )
    d_pre = (d_act * gelu_slope(pre)).astype(jnp.bfloat16)
    d_norm = lax.psum_scatter(
        jnp.dot(d_pre, w_first, preferred_element_type=jnp.float32).astype(jnp.bfloat16),
        "mp",
        scatter_dimension=0,
        tiled=True,
    ).astype(jnp.float32)
    offset = lax.axis_index("mp") * local_rows
    own_scale = lax.dynamic_slice_in_dim(scale, offset, local_rows, 0)
    shard_x = x_bwd.astype(jnp.float32)
    push = d_norm * gain_row[None, :]
    mixed = jnp.mean(shard_x * push, axis=-1, keepdims=True)
    dx = (
        cot_local.astype(jnp.float32)
        + own_scale * push
        - shard_x * own_scale * own_scale * own_scale * mixed
    )
    passed_grad = shifted(dx.astype(jnp.bfloat16), "section", -1)
    term_out = lax.dot_general(
        act, rows_cot, (((0,), (0,)), ((), ())), preferred_element_type=jnp.float32
    )
    term_in = lax.dot_general(
        d_pre, normed, (((0,), (0,)), ((), ())), preferred_element_type=jnp.float32
    )
    sum_in, sum_out = (
        lax.psum_scatter(
            term_in.astype(jnp.bfloat16), "dp", scatter_dimension=1, tiled=True
        ).astype(jnp.float32),
        lax.psum_scatter(
            term_out.astype(jnp.bfloat16), "dp", scatter_dimension=1, tiled=True
        ).astype(jnp.float32),
    )
    return (
        passed_fwd[None],
        passed_grad[None],
        sum_in.astype(jnp.bfloat16)[None],
        sum_out.astype(jnp.bfloat16)[None],
    )


MESH = pl.DeviceIdType.MESH
NT = (((1,), (1,)), ((), ()))
TN = (((0,), (0,)), ((), ()))
DIAG, DIRECT, SECOND, OWN = range(4)
OUT, IN = range(2)


def tile_of(total, most):
    size = min(total, most)
    while total % size:
        size //= 2
    return size


def relay_kernel(
    fwd_hbm, stash_hbm, cot_hbm, win_hbm, wout_hbm, gain_ref,
    pass_fwd, pass_grad, gin_ref, gout_ref,
    xs, xc, xf, nb, nf, win, wout, slope, act_t, dpre_t, act, parts, landed,
    mp_out, mp_in, own_terms, z_out,
    load_sem, mp_send, mp_recv, rs_send, rs_recv, z_send, z_recv,
):
    rows = stash_hbm.shape[0]
    hid, width = win_hbm.shape
    half = hid // 2
    cols = gin_ref.shape[1]
    n_sec = lax.axis_size("section")
    sec, dp, mp = lax.axis_index("section"), lax.axis_index("dp"), lax.axis_index("mp")
    y, x = lax.div(dp, 2), lax.rem(dp, 2)
    flip_x, flip_y = y * 2 + (1 - x), (1 - y) * 2 + x
    across = (1 - y) * 2 + (1 - x)
    peer = {"mp": 1 - mp}
    after, before = {"section": lax.rem(sec + 1, n_sec)}, {"section": lax.rem(sec + n_sec - 1, n_sec)}

    own, other = pl.ds(0, rows), pl.ds(rows, rows)
    loads = [
        pltpu.make_async_copy(stash_hbm, xs.at[own], load_sem.at[0]),
        pltpu.make_async_copy(win_hbm, win, load_sem.at[1]),
        pltpu.make_async_copy(cot_hbm, xc.at[own], load_sem.at[2]),
        pltpu.make_async_copy(wout_hbm, wout, load_sem.at[3]),
        pltpu.make_async_copy(fwd_hbm, xf.at[own], load_sem.at[4]),
    ]
    for load in loads:
        load.start()

    barrier = pltpu.get_barrier_semaphore()
    for target in (peer, {"dp": flip_x}, {"dp": flip_y}, after, before):
        pl.semaphore_signal(barrier, inc=1, device_id=target, device_id_type=MESH)
    pl.semaphore_wait(barrier, 5)

    def remote(src, dst, send, recv, target):
        copy = pltpu.make_async_remote_copy(
            src_ref=src, dst_ref=dst, send_sem=send, recv_sem=recv,
            device_id=target, device_id_type=MESH,
        )
        copy.start()
        return copy

    swaps = [
        remote(src, dst.at[other], mp_send.at[i], mp_recv.at[i], peer)
        for i, (src, dst) in enumerate(((stash_hbm, xs), (cot_hbm, xc), (fwd_hbm, xf)))
    ]

    gain = gain_ref[...]
    step = tile_of(rows, 64)

    def normalise(source, target, first):
        def body(i, carry):
            at = pl.ds(pl.multiple_of(first + i * step, step), step)
            v = source[at, :].astype(jnp.float32)
            r = lax.rsqrt(jnp.mean(v * v, axis=-1, keepdims=True) + norm_eps)
            target[at, :] = (v * r * gain).astype(jnp.bfloat16)
            return carry

        lax.fori_loop(0, rows // step, body, 0)

    block = tile_of(half, 256)

    def backward_pre(slot, first, count):
        def body(i, carry):
            at = pl.ds(pl.multiple_of(first + i * block, block), block)
            v = lax.dot_general(
                win[at, :], nb[slot, :], NT, preferred_element_type=jnp.float32
            )
            square = v * v
            t = jnp.tanh(gelu_coef * (v + 0.044715 * square * v))
            act_t[at, slot] = (0.5 * v * (1.0 + t)).astype(jnp.bfloat16)
            slope[at, slot] = 0.5 * (1.0 + t) + 0.5 * v * (1.0 - t * t) * gelu_coef * (
                1.0 + 0.134145 * square
            )
            return carry

        lax.fori_loop(0, count // block, body, 0)

    def backward_slope(first, count):
        def body(i, carry):
            at = pl.ds(pl.multiple_of(first + i * block, block), block)
            d_act = lax.dot_general(
                wout[at, :], xc[...], NT, preferred_element_type=jnp.float32
            )
            dpre_t[at, :] = (d_act * slope[at, :]).astype(jnp.bfloat16)
            return carry

        lax.fori_loop(0, count // block, body, 0)

    owners = (
        (across, flip_x, flip_y, dp),
        (across, flip_y, flip_x, dp),
    )
    nearest = (({"dp": flip_x}, {"dp": flip_y}), ({"dp": flip_y}, {"dp": flip_x}))
    halves = [pl.ds(0, half), pl.ds(half, half)]
    operands = {OUT: (act_t, xc), IN: (dpre_t, nb)}

    def product(g, h, kind):
        left, right = operands[g]
        at = pl.ds(pl.multiple_of(owners[h][kind] * cols, cols), cols)
        parts[g, h, kind] = jnp.dot(
            left[halves[h], :], right[:, at], preferred_element_type=jnp.float32
        ).astype(jnp.bfloat16)

    sent = {}

    def send(g, h, kind):
        sent[g, h, kind] = remote(
            parts.at[g, h, kind], landed.at[g, h, kind],
            rs_send.at[g, h, kind], rs_recv.at[g, h, kind],
            nearest[h][1 if kind == SECOND else 0],
        )

    loads[0].wait()
    normalise(xs, nb, 0)
    loads[1].wait()
    backward_pre(own, 0, hid)
    swaps[0].wait_recv()
    normalise(xs, nb, rows)
    backward_pre(other, 0, half)
    loads[2].wait()
    swaps[1].wait_recv()
    product(OUT, 0, DIAG)
    send(OUT, 0, DIAG)
    backward_pre(other, half, half)
    product(OUT, 1, DIAG)
    send(OUT, 1, DIAG)
    for h in range(2):
        product(OUT, h, DIRECT)
        send(OUT, h, DIRECT)

    loads[3].wait()
    for h in range(2):
        backward_slope(h * half, half)
        product(IN, h, DIAG)
        send(IN, h, DIAG)
    for h in range(2):
        product(IN, h, DIRECT)
        send(IN, h, DIRECT)

    def d_norm(slot):
        return lax.dot_general(
            dpre_t[:, slot], win[...], TN, preferred_element_type=jnp.float32
        ).astype(jnp.bfloat16)

    mp_out[0] = d_norm(other)
    swap_grad = remote(mp_out.at[0], mp_in.at[0], mp_send.at[3], mp_recv.at[3], peer)
    own_terms[0] = d_norm(own)

    loads[4].wait()

    def forward(slot):
        def body(i, carry):
            at = pl.ds(pl.multiple_of(i * block, block), block)
            v = lax.dot_general(
                nf[slot, :], win[at, :], NT, preferred_element_type=jnp.float32
            )
            t = jnp.tanh(gelu_coef * (v + 0.044715 * v * v * v))
            act[:, at] = (0.5 * v * (1.0 + t)).astype(jnp.bfloat16)
            return carry

        lax.fori_loop(0, hid // block, body, 0)
        return jnp.dot(
            act[...], wout[...], preferred_element_type=jnp.float32
        ).astype(jnp.bfloat16)

    swap_grad.wait_recv()

    def finish_grad(i, carry):
        at = pl.ds(pl.multiple_of(i * step, step), step)
        v = xs[at, :].astype(jnp.float32)
        r = lax.rsqrt(jnp.mean(v * v, axis=-1, keepdims=True) + norm_eps)
        push = (own_terms[0, at, :].astype(jnp.float32) + mp_in[0, at, :].astype(jnp.float32)) * gain
        mixed = jnp.mean(v * push, axis=-1, keepdims=True)
        dx = xc[at, :].astype(jnp.float32) + r * push - v * (r * r * r * mixed)
        z_out[0, at, :] = dx.astype(jnp.bfloat16)
        return carry

    lax.fori_loop(0, rows // step, finish_grad, 0)
    relay_grad = remote(z_out.at[0], pass_grad, z_send.at[0], z_recv.at[0], before)

    swaps[2].wait_recv()
    normalise(xf, nf, rows)
    mp_out[1] = forward(other)
    swap_branch = remote(mp_out.at[1], mp_in.at[1], mp_send.at[4], mp_recv.at[4], peer)
    normalise(xf, nf, 0)
    own_terms[1] = forward(own)
    swap_branch.wait_recv()

    def finish_forward(i, carry):
        at = pl.ds(pl.multiple_of(i * step, step), step)
        branch = own_terms[1, at, :].astype(jnp.float32) + mp_in[1, at, :].astype(jnp.float32)
        z_out[1, at, :] = (xf[at, :].astype(jnp.float32) + branch).astype(jnp.bfloat16)
        return carry

    lax.fori_loop(0, rows // step, finish_forward, 0)
    relay_fwd = remote(z_out.at[1], pass_fwd, z_send.at[1], z_recv.at[1], after)

    for g in (OUT, IN):
        for h in range(2):
            product(g, h, SECOND)
        for h in range(2):
            sent[g, h, DIAG].wait_recv()
            parts[g, h, SECOND] = (
                parts[g, h, SECOND].astype(jnp.float32) + landed[g, h, DIAG].astype(jnp.float32)
            ).astype(jnp.bfloat16)
            send(g, h, SECOND)
        for h in range(2):
            product(g, h, OWN)
    for g, result in ((OUT, gout_ref), (IN, gin_ref)):
        for h in range(2):
            sent[g, h, DIRECT].wait_recv()
            sent[g, h, SECOND].wait_recv()
            result[halves[h], :] = (
                parts[g, h, OWN].astype(jnp.float32)
                + landed[g, h, DIRECT].astype(jnp.float32)
                + landed[g, h, SECOND].astype(jnp.float32)
            ).astype(jnp.bfloat16)

    relay_grad.wait_recv()
    relay_fwd.wait_recv()
    for copy in [*swaps, swap_grad, swap_branch, relay_grad, relay_fwd, *sent.values()]:
        copy.wait_send()


def relay_on_device(fwd_in, stash, cot, w_in, w_out, gain):
    rows, width = stash.shape[1:]
    hid = w_in.shape[1]
    tokens = rows * lax.axis_size("mp")
    cols = width // lax.axis_size("dp")
    half = hid // 2
    bf16 = jnp.bfloat16
    vmem = pl.BlockSpec(memory_space=pltpu.VMEM)
    hbm = pl.BlockSpec(memory_space=pl.ANY)
    shape = jax.ShapeDtypeStruct
    results = pl.pallas_call(
        relay_kernel,
        out_shape=(
            shape((rows, width), bf16), shape((rows, width), bf16),
            shape((hid, cols), bf16), shape((hid, cols), bf16),
        ),
        in_specs=[hbm] * 5 + [vmem],
        out_specs=(vmem,) * 4,
        scratch_shapes=[
            pltpu.VMEM((tokens, width), bf16),
            pltpu.VMEM((tokens, width), bf16),
            pltpu.VMEM((tokens, width), bf16),
            pltpu.VMEM((tokens, width), bf16),
            pltpu.VMEM((tokens, width), bf16),
            pltpu.VMEM((hid, width), bf16),
            pltpu.VMEM((hid, width), bf16),
            pltpu.VMEM((hid, tokens), jnp.float32),
            pltpu.VMEM((hid, tokens), bf16),
            pltpu.VMEM((hid, tokens), bf16),
            pltpu.VMEM((rows, hid), bf16),
            pltpu.VMEM((2, 2, 4, half, cols), bf16),
            pltpu.VMEM((2, 2, 3, half, cols), bf16),
            pltpu.VMEM((2, rows, width), bf16),
            pltpu.VMEM((2, rows, width), bf16),
            pltpu.VMEM((2, rows, width), bf16),
            pltpu.VMEM((2, rows, width), bf16),
            pltpu.SemaphoreType.DMA((5,)),
            pltpu.SemaphoreType.DMA((5,)),
            pltpu.SemaphoreType.DMA((5,)),
            pltpu.SemaphoreType.DMA((2, 2, 3)),
            pltpu.SemaphoreType.DMA((2, 2, 3)),
            pltpu.SemaphoreType.DMA((2,)),
            pltpu.SemaphoreType.DMA((2,)),
        ],
        compiler_params=pltpu.CompilerParams(
            collective_id=0, has_side_effects=True, vmem_limit_bytes=56 * 2**20
        ),
    )(fwd_in[0], stash[0], cot[0], w_in[0], w_out[0], gain)
    return tuple(r[None] for r in results)


def fits_relay(mesh):
    return mesh.shape["dp"] == 4 and mesh.shape["mp"] == 2 and mesh.shape["section"] > 1


def solution(mesh):
    in_specs = (
        P("section", ("dp", "mp"), None),
        P("section", ("dp", "mp"), None),
        P("section", ("dp", "mp"), None),
        P("section", "mp", None),
        P("section", "mp", None),
        P("section", None),
    )
    out_specs = (
        P("section", ("dp", "mp"), None),
        P("section", ("dp", "mp"), None),
        P("section", "mp", "dp"),
        P("section", "mp", "dp"),
    )
    return jax.shard_map(
        relay_on_device if fits_relay(mesh) else on_device,
        mesh=mesh,
        in_specs=in_specs,
        out_specs=out_specs,
        check_vma=False,
    )
```

```python
import jax
import jax.numpy as jnp
from jax import lax
from jax.experimental import pallas as pl
from jax.experimental.pallas import tpu as pltpu
from jax.sharding import PartitionSpec as P

norm_eps = 1e-05
gelu_coef = 0.7978845608


def shifted(x, axis, by):
    length = lax.axis_size(axis)
    return lax.ppermute(x, axis, [(i, (i + by) % length) for i in range(length)])


def gelu_value(v):
    inner = jnp.tanh(gelu_coef * (v + 0.044715 * v * v * v))
    return 0.5 * v * (1.0 + inner)


def gelu_slope(v):
    inner = jnp.tanh(gelu_coef * (v + 0.044715 * v * v * v))
    return 0.5 * (1.0 + inner) + 0.5 * v * (1.0 - inner * inner) * gelu_coef * (
        1.0 + 0.134145 * v * v
    )


def prepare(x, w_first, gain_row):
    xf = x.astype(jnp.float32)
    scale = lax.rsqrt(jnp.mean(xf * xf, axis=-1, keepdims=True) + norm_eps)
    normed = (xf * scale * gain_row[None, :]).astype(jnp.bfloat16)
    pre = lax.dot_general(
        normed, w_first, (((1,), (1,)), ((), ())), preferred_element_type=jnp.float32
    )
    act = gelu_value(pre).astype(jnp.bfloat16)
    return (scale, normed, pre, act)


def on_device(fwd_in, stash, cot, w_in, w_out, gain):
    x_fwd = fwd_in[0]
    x_bwd = stash[0]
    cot_local = cot[0]
    w_first = w_in[0]
    w_second = w_out[0]
    gain_row = gain[0]
    local_rows = x_fwd.shape[0]
    scale, normed, pre, act = prepare(
        lax.all_gather(x_fwd, "mp", axis=0, tiled=True), w_first, gain_row
    )
    terms = jnp.dot(act, w_second, preferred_element_type=jnp.float32)
    branch = lax.psum_scatter(
        terms.astype(jnp.bfloat16), "mp", scatter_dimension=0, tiled=True
    ).astype(jnp.float32)
    out = (x_fwd.astype(jnp.float32) + branch).astype(jnp.bfloat16)
    passed_fwd = shifted(out, "section", 1)
    rows_x, rows_cot = (
        lax.all_gather(x_bwd, "mp", axis=0, tiled=True),
        lax.all_gather(cot_local, "mp", axis=0, tiled=True),
    )
    scale, normed, pre, act = prepare(rows_x, w_first, gain_row)
    d_act = lax.dot_general(
        rows_cot, w_second, (((1,), (1,)), ((), ())), preferred_element_type=jnp.float32
    )
    d_pre = (d_act * gelu_slope(pre)).astype(jnp.bfloat16)
    d_norm = lax.psum_scatter(
        jnp.dot(d_pre, w_first, preferred_element_type=jnp.float32).astype(jnp.bfloat16),
        "mp",
        scatter_dimension=0,
        tiled=True,
    ).astype(jnp.float32)
    offset = lax.axis_index("mp") * local_rows
    own_scale = lax.dynamic_slice_in_dim(scale, offset, local_rows, 0)
    shard_x = x_bwd.astype(jnp.float32)
    push = d_norm * gain_row[None, :]
    mixed = jnp.mean(shard_x * push, axis=-1, keepdims=True)
    dx = (
        cot_local.astype(jnp.float32)
        + own_scale * push
        - shard_x * own_scale * own_scale * own_scale * mixed
    )
    passed_grad = shifted(dx.astype(jnp.bfloat16), "section", -1)
    term_out = lax.dot_general(
        act, rows_cot, (((0,), (0,)), ((), ())), preferred_element_type=jnp.float32
    )
    term_in = lax.dot_general(
        d_pre, normed, (((0,), (0,)), ((), ())), preferred_element_type=jnp.float32
    )
    sum_in, sum_out = (
        lax.psum_scatter(
            term_in.astype(jnp.bfloat16), "dp", scatter_dimension=1, tiled=True
        ).astype(jnp.float32),
        lax.psum_scatter(
            term_out.astype(jnp.bfloat16), "dp", scatter_dimension=1, tiled=True
        ).astype(jnp.float32),
    )
    return (
        passed_fwd[None],
        passed_grad[None],
        sum_in.astype(jnp.bfloat16)[None],
        sum_out.astype(jnp.bfloat16)[None],
    )


MESH = pl.DeviceIdType.MESH
vmem_bytes = 67_043_328
NT = (((1,), (1,)), ((), ()))
TN = (((0,), (0,)), ((), ()))
DIAG, DIRECT, SECOND, OWN = range(4)
OUT, IN = range(2)


def tile_of(total, most):
    size = min(total, most)
    while total % size:
        size //= 2
    return size


def start_remote(src, dst, send, recv, target):
    copy = pltpu.make_async_remote_copy(
        src_ref=src, dst_ref=dst, send_sem=send, recv_sem=recv,
        device_id=target, device_id_type=MESH,
    )
    copy.start()
    return copy


def greet(targets):
    barrier = pltpu.get_barrier_semaphore()
    for target in targets:
        pl.semaphore_signal(barrier, inc=1, device_id=target, device_id_type=MESH)
    return barrier


def swap_kernel(
    fwd_hbm, stash_hbm, cot_hbm, win_hbm, wout_hbm,
    xs, xc, xf, win, wout,
    load_sem, send_sem, recv_sem,
):
    rows = stash_hbm.shape[0]
    peer = {"mp": 1 - lax.axis_index("mp")}
    barrier = greet([peer])
    own, other = pl.ds(0, rows), pl.ds(rows, rows)
    shared = ((stash_hbm, xs), (cot_hbm, xc), (fwd_hbm, xf))
    pairs = [(src, dst.at[own]) for src, dst in shared] + [(win_hbm, win), (wout_hbm, wout)]
    loads = [
        pltpu.make_async_copy(src, dst, load_sem.at[i]) for i, (src, dst) in enumerate(pairs)
    ]
    pl.semaphore_wait(barrier, 1)
    swaps = [
        start_remote(src, dst.at[other], send_sem.at[i], recv_sem.at[i], peer)
        for i, (src, dst) in enumerate(shared)
    ]
    for load in loads:
        load.start()
    for load in loads:
        load.wait()
    for swap in swaps:
        swap.wait()


def write_kernel(a, b, c, d, a_out, b_out, c_out, d_out, sems):
    copies = [
        pltpu.make_async_copy(src, dst, sems.at[i])
        for i, (src, dst) in enumerate(((a, a_out), (b, b_out), (c, c_out), (d, d_out)))
    ]
    for copy in copies:
        copy.start()
    for copy in copies:
        copy.wait()


def relay_kernel(
    xs, xc, xf, win, wout, gain_ref,
    pass_fwd, pass_grad, gin_ref, gout_ref,
    nb, nf, slope, act_t, dpre_t, act, parts, landed,
    mp_out, mp_in, own_terms, z_out,
    mp_send, mp_recv, rs_send, rs_recv, z_send, z_recv,
):
    rows = pass_fwd.shape[0]
    hid, width = win.shape
    half = hid // 2
    cols = gin_ref.shape[1]
    n_sec = lax.axis_size("section")
    sec, dp, mp = lax.axis_index("section"), lax.axis_index("dp"), lax.axis_index("mp")
    y, x = lax.div(dp, 2), lax.rem(dp, 2)
    flip_x, flip_y = y * 2 + (1 - x), (1 - y) * 2 + x
    across = (1 - y) * 2 + (1 - x)
    peer = {"mp": 1 - mp}
    after, before = {"section": lax.rem(sec + 1, n_sec)}, {"section": lax.rem(sec + n_sec - 1, n_sec)}
    barrier = greet([after, before, {"dp": flip_x}, {"dp": flip_y}, peer])

    own, other = pl.ds(0, rows), pl.ds(rows, rows)
    gain = gain_ref[...]
    step = tile_of(rows, 64)

    def normalise(source, target, first):
        def body(i, carry):
            at = pl.ds(pl.multiple_of(first + i * step, step), step)
            v = source[at, :].astype(jnp.float32)
            r = lax.rsqrt(jnp.mean(v * v, axis=-1, keepdims=True) + norm_eps)
            target[at, :] = (v * r * gain).astype(jnp.bfloat16)
            return carry

        lax.fori_loop(0, rows // step, body, 0)

    block = tile_of(half, 256)

    def backward_pre(first, count):
        def body(i, carry):
            at = pl.ds(pl.multiple_of(first + i * block, block), block)
            v = lax.dot_general(
                win[at, :], nb[...], NT, preferred_element_type=jnp.float32
            )
            square = v * v
            t = jnp.tanh(gelu_coef * (v + 0.044715 * square * v))
            act_t[at, :] = (0.5 * v * (1.0 + t)).astype(jnp.bfloat16)
            slope[at, :] = 0.5 * (1.0 + t) + 0.5 * v * (1.0 - t * t) * gelu_coef * (
                1.0 + 0.134145 * square
            )
            return carry

        lax.fori_loop(0, count // block, body, 0)

    def backward_slope(first, count):
        def body(i, carry):
            at = pl.ds(pl.multiple_of(first + i * block, block), block)
            d_act = lax.dot_general(
                wout[at, :], xc[...], NT, preferred_element_type=jnp.float32
            )
            dpre_t[at, :] = (d_act * slope[at, :]).astype(jnp.bfloat16)
            return carry

        lax.fori_loop(0, count // block, body, 0)

    owners = (
        (across, flip_x, flip_y, dp),
        (across, flip_y, flip_x, dp),
    )
    nearest = (({"dp": flip_x}, {"dp": flip_y}), ({"dp": flip_y}, {"dp": flip_x}))
    halves = [pl.ds(0, half), pl.ds(half, half)]
    operands = {OUT: (act_t, xc), IN: (dpre_t, nb)}

    def product(g, h, kind):
        left, right = operands[g]
        at = pl.ds(pl.multiple_of(owners[h][kind] * cols, cols), cols)
        parts[g, h, kind] = jnp.dot(
            left[halves[h], :], right[:, at], preferred_element_type=jnp.float32
        ).astype(jnp.bfloat16)

    sent = {}

    def send(g, h, kind):
        sent[g, h, kind] = start_remote(
            parts.at[g, h, kind], landed.at[g, h, kind],
            rs_send.at[g, h, kind], rs_recv.at[g, h, kind],
            nearest[h][1 if kind == SECOND else 0],
        )

    normalise(xs, nb, 0)
    normalise(xs, nb, rows)
    backward_pre(0, half)
    product(OUT, 0, DIAG)
    pl.semaphore_wait(barrier, 5)
    send(OUT, 0, DIAG)
    backward_pre(half, half)
    product(OUT, 1, DIAG)
    send(OUT, 1, DIAG)
    for h in range(2):
        product(OUT, h, DIRECT)
        send(OUT, h, DIRECT)

    for h in range(2):
        backward_slope(h * half, half)
        product(IN, h, DIAG)
        send(IN, h, DIAG)
    for h in range(2):
        product(IN, h, DIRECT)
        send(IN, h, DIRECT)

    def d_norm(slot):
        return lax.dot_general(
            dpre_t[:, slot], win[...], TN, preferred_element_type=jnp.float32
        ).astype(jnp.bfloat16)

    mp_out[0] = d_norm(other)
    swap_grad = start_remote(mp_out.at[0], mp_in.at[0], mp_send.at[0], mp_recv.at[0], peer)
    own_terms[0] = d_norm(own)


    def forward(slot):
        def body(i, carry):
            at = pl.ds(pl.multiple_of(i * block, block), block)
            v = lax.dot_general(
                nf[slot, :], win[at, :], NT, preferred_element_type=jnp.float32
            )
            t = jnp.tanh(gelu_coef * (v + 0.044715 * v * v * v))
            act[:, at] = (0.5 * v * (1.0 + t)).astype(jnp.bfloat16)
            return carry

        lax.fori_loop(0, hid // block, body, 0)
        return jnp.dot(
            act[...], wout[...], preferred_element_type=jnp.float32
        ).astype(jnp.bfloat16)

    swap_grad.wait_recv()

    def finish_grad(i, carry):
        at = pl.ds(pl.multiple_of(i * step, step), step)
        v = xs[at, :].astype(jnp.float32)
        r = lax.rsqrt(jnp.mean(v * v, axis=-1, keepdims=True) + norm_eps)
        push = (own_terms[0, at, :].astype(jnp.float32) + mp_in[0, at, :].astype(jnp.float32)) * gain
        mixed = jnp.mean(v * push, axis=-1, keepdims=True)
        dx = xc[at, :].astype(jnp.float32) + r * push - v * (r * r * r * mixed)
        z_out[0, at, :] = dx.astype(jnp.bfloat16)
        return carry

    lax.fori_loop(0, rows // step, finish_grad, 0)
    relay_grad = start_remote(z_out.at[0], pass_grad, z_send.at[0], z_recv.at[0], before)

    normalise(xf, nf, rows)
    mp_out[1] = forward(other)
    swap_branch = start_remote(mp_out.at[1], mp_in.at[1], mp_send.at[1], mp_recv.at[1], peer)
    normalise(xf, nf, 0)
    own_terms[1] = forward(own)
    swap_branch.wait_recv()

    def finish_forward(i, carry):
        at = pl.ds(pl.multiple_of(i * step, step), step)
        branch = own_terms[1, at, :].astype(jnp.float32) + mp_in[1, at, :].astype(jnp.float32)
        z_out[1, at, :] = (xf[at, :].astype(jnp.float32) + branch).astype(jnp.bfloat16)
        return carry

    lax.fori_loop(0, rows // step, finish_forward, 0)
    relay_fwd = start_remote(z_out.at[1], pass_fwd, z_send.at[1], z_recv.at[1], after)

    for g in (OUT, IN):
        for h in range(2):
            product(g, h, SECOND)
        for h in range(2):
            sent[g, h, DIAG].wait_recv()
            parts[g, h, SECOND] = (
                parts[g, h, SECOND].astype(jnp.float32) + landed[g, h, DIAG].astype(jnp.float32)
            ).astype(jnp.bfloat16)
            send(g, h, SECOND)
        for h in range(2):
            product(g, h, OWN)
    for g, result in ((OUT, gout_ref), (IN, gin_ref)):
        for h in range(2):
            sent[g, h, DIRECT].wait_recv()
            sent[g, h, SECOND].wait_recv()
            result[halves[h], :] = (
                parts[g, h, OWN].astype(jnp.float32)
                + landed[g, h, DIRECT].astype(jnp.float32)
                + landed[g, h, SECOND].astype(jnp.float32)
            ).astype(jnp.bfloat16)

    relay_grad.wait_recv()
    relay_fwd.wait_recv()
    for copy in [swap_grad, swap_branch, relay_grad, relay_fwd, *sent.values()]:
        copy.wait_send()


def relay_on_device(fwd_in, stash, cot, w_in, w_out, gain):
    rows, width = stash.shape[1:]
    hid = w_in.shape[1]
    tokens = rows * lax.axis_size("mp")
    cols = width // lax.axis_size("dp")
    half = hid // 2
    bf16 = jnp.bfloat16
    vmem = pl.BlockSpec(memory_space=pltpu.VMEM)
    hbm = pl.BlockSpec(memory_space=pl.ANY)
    dma = pltpu.SemaphoreType.DMA
    held = (tokens * 3 + hid * 2) * width * jnp.dtype(bf16).itemsize
    loaded = pl.pallas_call(
        swap_kernel,
        out_shape=(pltpu.VMEM((tokens, width), bf16),) * 3
        + (pltpu.VMEM((hid, width), bf16),) * 2,
        in_specs=[hbm] * 5,
        out_specs=(vmem,) * 5,
        scratch_shapes=[dma((5,)), dma((3,)), dma((3,))],
        compiler_params=pltpu.CompilerParams(
            collective_id=0, has_side_effects=True,
            vmem_limit_bytes=vmem_bytes - held - 2**17,
        ),
    )(fwd_in[0], stash[0], cot[0], w_in[0], w_out[0])
    results = pl.pallas_call(
        relay_kernel,
        out_shape=(pltpu.VMEM((rows, width), bf16),) * 2 + (pltpu.VMEM((hid, cols), bf16),) * 2,
        in_specs=[vmem] * 6,
        out_specs=(vmem,) * 4,
        scratch_shapes=[
            pltpu.VMEM((tokens, width), bf16),
            pltpu.VMEM((tokens, width), bf16),
            pltpu.VMEM((hid, tokens), jnp.float32),
            pltpu.VMEM((hid, tokens), bf16),
            pltpu.VMEM((hid, tokens), bf16),
            pltpu.VMEM((rows, hid), bf16),
            pltpu.VMEM((2, 2, 4, half, cols), bf16),
            pltpu.VMEM((2, 2, 3, half, cols), bf16),
            pltpu.VMEM((2, rows, width), bf16),
            pltpu.VMEM((2, rows, width), bf16),
            pltpu.VMEM((2, rows, width), bf16),
            pltpu.VMEM((2, rows, width), bf16),
            dma((2,)),
            dma((2,)),
            dma((2, 2, 3)),
            dma((2, 2, 3)),
            dma((2,)),
            dma((2,)),
        ],
        compiler_params=pltpu.CompilerParams(
            collective_id=1, has_side_effects=True, vmem_limit_bytes=40 * 2**20
        ),
    )(*loaded, gain)
    results = pl.pallas_call(
        write_kernel,
        out_shape=tuple(jax.ShapeDtypeStruct(r.shape, r.dtype) for r in results),
        in_specs=[vmem] * 4,
        out_specs=(hbm,) * 4,
        scratch_shapes=[dma((4,))],
        compiler_params=pltpu.CompilerParams(vmem_limit_bytes=4 * 2**20),
    )(*results)
    return tuple(r[None] for r in results)


def fits_relay(mesh):
    return mesh.shape["dp"] == 4 and mesh.shape["mp"] == 2 and mesh.shape["section"] > 1


def solution(mesh):
    in_specs = (
        P("section", ("dp", "mp"), None),
        P("section", ("dp", "mp"), None),
        P("section", ("dp", "mp"), None),
        P("section", "mp", None),
        P("section", "mp", None),
        P("section", None),
    )
    out_specs = (
        P("section", ("dp", "mp"), None),
        P("section", ("dp", "mp"), None),
        P("section", "mp", "dp"),
        P("section", "mp", "dp"),
    )
    return jax.shard_map(
        relay_on_device if fits_relay(mesh) else on_device,
        mesh=mesh,
        in_specs=in_specs,
        out_specs=out_specs,
        check_vma=False,
    )
```

```python
import jax
import jax.numpy as jnp
from jax import lax
from jax.experimental import pallas as pl
from jax.experimental.pallas import tpu as pltpu
from jax.sharding import PartitionSpec as P

norm_eps = 1e-05
gelu_coef = 0.7978845608


def shifted(x, axis, by):
    length = lax.axis_size(axis)
    return lax.ppermute(x, axis, [(i, (i + by) % length) for i in range(length)])


def gelu_value(v):
    inner = jnp.tanh(gelu_coef * (v + 0.044715 * v * v * v))
    return 0.5 * v * (1.0 + inner)


def gelu_slope(v):
    inner = jnp.tanh(gelu_coef * (v + 0.044715 * v * v * v))
    return 0.5 * (1.0 + inner) + 0.5 * v * (1.0 - inner * inner) * gelu_coef * (
        1.0 + 0.134145 * v * v
    )


def prepare(x, w_first, gain_row):
    xf = x.astype(jnp.float32)
    scale = lax.rsqrt(jnp.mean(xf * xf, axis=-1, keepdims=True) + norm_eps)
    normed = (xf * scale * gain_row[None, :]).astype(jnp.bfloat16)
    pre = lax.dot_general(
        normed, w_first, (((1,), (1,)), ((), ())), preferred_element_type=jnp.float32
    )
    act = gelu_value(pre).astype(jnp.bfloat16)
    return (scale, normed, pre, act)


def on_device(fwd_in, stash, cot, w_in, w_out, gain):
    x_fwd = fwd_in[0]
    x_bwd = stash[0]
    cot_local = cot[0]
    w_first = w_in[0]
    w_second = w_out[0]
    gain_row = gain[0]
    local_rows = x_fwd.shape[0]
    scale, normed, pre, act = prepare(
        lax.all_gather(x_fwd, "mp", axis=0, tiled=True), w_first, gain_row
    )
    terms = jnp.dot(act, w_second, preferred_element_type=jnp.float32)
    branch = lax.psum_scatter(
        terms.astype(jnp.bfloat16), "mp", scatter_dimension=0, tiled=True
    ).astype(jnp.float32)
    out = (x_fwd.astype(jnp.float32) + branch).astype(jnp.bfloat16)
    passed_fwd = shifted(out, "section", 1)
    rows_x, rows_cot = (
        lax.all_gather(x_bwd, "mp", axis=0, tiled=True),
        lax.all_gather(cot_local, "mp", axis=0, tiled=True),
    )
    scale, normed, pre, act = prepare(rows_x, w_first, gain_row)
    d_act = lax.dot_general(
        rows_cot, w_second, (((1,), (1,)), ((), ())), preferred_element_type=jnp.float32
    )
    d_pre = (d_act * gelu_slope(pre)).astype(jnp.bfloat16)
    d_norm = lax.psum_scatter(
        jnp.dot(d_pre, w_first, preferred_element_type=jnp.float32).astype(jnp.bfloat16),
        "mp",
        scatter_dimension=0,
        tiled=True,
    ).astype(jnp.float32)
    offset = lax.axis_index("mp") * local_rows
    own_scale = lax.dynamic_slice_in_dim(scale, offset, local_rows, 0)
    shard_x = x_bwd.astype(jnp.float32)
    push = d_norm * gain_row[None, :]
    mixed = jnp.mean(shard_x * push, axis=-1, keepdims=True)
    dx = (
        cot_local.astype(jnp.float32)
        + own_scale * push
        - shard_x * own_scale * own_scale * own_scale * mixed
    )
    passed_grad = shifted(dx.astype(jnp.bfloat16), "section", -1)
    term_out = lax.dot_general(
        act, rows_cot, (((0,), (0,)), ((), ())), preferred_element_type=jnp.float32
    )
    term_in = lax.dot_general(
        d_pre, normed, (((0,), (0,)), ((), ())), preferred_element_type=jnp.float32
    )
    sum_in, sum_out = (
        lax.psum_scatter(
            term_in.astype(jnp.bfloat16), "dp", scatter_dimension=1, tiled=True
        ).astype(jnp.float32),
        lax.psum_scatter(
            term_out.astype(jnp.bfloat16), "dp", scatter_dimension=1, tiled=True
        ).astype(jnp.float32),
    )
    return (
        passed_fwd[None],
        passed_grad[None],
        sum_in.astype(jnp.bfloat16)[None],
        sum_out.astype(jnp.bfloat16)[None],
    )


MESH = pl.DeviceIdType.MESH
vmem_bytes = 67_043_328
NT = (((1,), (1,)), ((), ()))
TN = (((0,), (0,)), ((), ()))
DIAG, DIRECT, SECOND, OWN = range(4)
OUT, IN = range(2)


def tile_of(total, most):
    size = min(total, most)
    while total % size:
        size //= 2
    return size


def start_remote(src, dst, send, recv, target):
    copy = pltpu.make_async_remote_copy(
        src_ref=src, dst_ref=dst, send_sem=send, recv_sem=recv,
        device_id=target, device_id_type=MESH,
    )
    copy.start()
    return copy


def greet(targets):
    barrier = pltpu.get_barrier_semaphore()
    for target in targets:
        pl.semaphore_signal(barrier, inc=1, device_id=target, device_id_type=MESH)
    return barrier


def swap_kernel(
    fwd_hbm, stash_hbm, cot_hbm, win_hbm, wout_hbm,
    xs, xc, xf, win, wout,
    load_sem, send_sem, recv_sem,
):
    rows = stash_hbm.shape[0]
    peer = {"mp": 1 - lax.axis_index("mp")}
    barrier = greet([peer])
    own, other = pl.ds(0, rows), pl.ds(rows, rows)
    shared = ((stash_hbm, xs), (cot_hbm, xc))
    whole = ((win_hbm, win), (fwd_hbm, xf), (wout_hbm, wout))
    pairs = [*((src, dst.at[own]) for src, dst in shared), *whole]
    loads = [
        pltpu.make_async_copy(src, dst, load_sem.at[i]) for i, (src, dst) in enumerate(pairs)
    ]
    pl.semaphore_wait(barrier, 1)
    swaps = [
        start_remote(src, dst.at[other], send_sem.at[i], recv_sem.at[i], peer)
        for i, (src, dst) in enumerate(shared)
    ]
    for load in loads:
        load.start()
    for load in loads:
        load.wait()
    for swap in swaps:
        swap.wait()


def write_kernel(a, b, c, d, a_out, b_out, c_out, d_out, sems):
    copies = [
        pltpu.make_async_copy(src, dst, sems.at[i])
        for i, (src, dst) in enumerate(((a, a_out), (b, b_out), (c, c_out), (d, d_out)))
    ]
    for copy in copies:
        copy.start()
    for copy in copies:
        copy.wait()


def relay_kernel(
    xs, xc, xf, win, wout, gain_ref,
    pass_fwd, pass_grad, gin_ref, gout_ref,
    xf_peer, nb, nf, slope, act_t, dpre_t, act, parts, landed,
    mp_out, mp_in, own_terms, z_out,
    mp_send, mp_recv, rs_send, rs_recv, z_send, z_recv,
):
    rows = pass_fwd.shape[0]
    hid, width = win.shape
    half = hid // 2
    cols = gin_ref.shape[1]
    n_sec = lax.axis_size("section")
    sec, dp, mp = lax.axis_index("section"), lax.axis_index("dp"), lax.axis_index("mp")
    y, x = lax.div(dp, 2), lax.rem(dp, 2)
    flip_x, flip_y = y * 2 + (1 - x), (1 - y) * 2 + x
    across = (1 - y) * 2 + (1 - x)
    peer = {"mp": 1 - mp}
    after, before = {"section": lax.rem(sec + 1, n_sec)}, {"section": lax.rem(sec + n_sec - 1, n_sec)}
    barrier = greet([after, before, {"dp": flip_x}, {"dp": flip_y}, peer])

    own, other = pl.ds(0, rows), pl.ds(rows, rows)
    gain = gain_ref[...]
    step = tile_of(rows, 64)

    def normalise(source, target, first, skip=0):
        def body(i, carry):
            at = pl.ds(pl.multiple_of(first + i * step, step), step)
            v = source[pl.ds(pl.multiple_of(first - skip + i * step, step), step), :].astype(jnp.float32)
            r = lax.rsqrt(jnp.mean(v * v, axis=-1, keepdims=True) + norm_eps)
            target[at, :] = (v * r * gain).astype(jnp.bfloat16)
            return carry

        lax.fori_loop(0, rows // step, body, 0)

    block = tile_of(half, 256)

    def backward_pre(first, count):
        def body(i, carry):
            at = pl.ds(pl.multiple_of(first + i * block, block), block)
            v = lax.dot_general(
                win[at, :], nb[...], NT, preferred_element_type=jnp.float32
            )
            square = v * v
            t = jnp.tanh(gelu_coef * (v + 0.044715 * square * v))
            act_t[at, :] = (0.5 * v * (1.0 + t)).astype(jnp.bfloat16)
            slope[at, :] = 0.5 * (1.0 + t) + 0.5 * v * (1.0 - t * t) * gelu_coef * (
                1.0 + 0.134145 * square
            )
            return carry

        lax.fori_loop(0, count // block, body, 0)

    def backward_slope(first, count):
        def body(i, carry):
            at = pl.ds(pl.multiple_of(first + i * block, block), block)
            d_act = lax.dot_general(
                wout[at, :], xc[...], NT, preferred_element_type=jnp.float32
            )
            dpre_t[at, :] = (d_act * slope[at, :]).astype(jnp.bfloat16)
            return carry

        lax.fori_loop(0, count // block, body, 0)

    owners = (
        (across, flip_x, flip_y, dp),
        (across, flip_y, flip_x, dp),
    )
    nearest = (({"dp": flip_x}, {"dp": flip_y}), ({"dp": flip_y}, {"dp": flip_x}))
    halves = [pl.ds(0, half), pl.ds(half, half)]
    operands = {OUT: (act_t, xc), IN: (dpre_t, nb)}

    def product(g, h, kind):
        left, right = operands[g]
        at = pl.ds(pl.multiple_of(owners[h][kind] * cols, cols), cols)
        parts[g, h, kind] = jnp.dot(
            left[halves[h], :], right[:, at], preferred_element_type=jnp.float32
        ).astype(jnp.bfloat16)

    sent = {}

    def send(g, h, kind):
        sent[g, h, kind] = start_remote(
            parts.at[g, h, kind], landed.at[g, h, kind],
            rs_send.at[g, h, kind], rs_recv.at[g, h, kind],
            nearest[h][1 if kind == SECOND else 0],
        )

    normalise(xs, nb, 0)
    normalise(xs, nb, rows)
    backward_pre(0, half)
    product(OUT, 0, DIAG)
    backward_pre(half, half)
    product(OUT, 1, DIAG)
    pl.semaphore_wait(barrier, 5)
    send(OUT, 0, DIAG)
    send(OUT, 1, DIAG)
    swap_fwd = start_remote(xf, xf_peer, mp_send.at[2], mp_recv.at[2], peer)
    for h in range(2):
        product(OUT, h, DIRECT)
        send(OUT, h, DIRECT)

    for h in range(2):
        backward_slope(h * half, half)
        product(IN, h, DIAG)
        send(IN, h, DIAG)
    for h in range(2):
        product(IN, h, DIRECT)
        send(IN, h, DIRECT)

    def d_norm(slot):
        return lax.dot_general(
            dpre_t[:, slot], win[...], TN, preferred_element_type=jnp.float32
        ).astype(jnp.bfloat16)

    mp_out[0] = d_norm(other)
    swap_grad = start_remote(mp_out.at[0], mp_in.at[0], mp_send.at[0], mp_recv.at[0], peer)
    own_terms[0] = d_norm(own)


    def forward(slot):
        def body(i, carry):
            at = pl.ds(pl.multiple_of(i * block, block), block)
            v = lax.dot_general(
                nf[slot, :], win[at, :], NT, preferred_element_type=jnp.float32
            )
            t = jnp.tanh(gelu_coef * (v + 0.044715 * v * v * v))
            act[:, at] = (0.5 * v * (1.0 + t)).astype(jnp.bfloat16)
            return carry

        lax.fori_loop(0, hid // block, body, 0)
        return jnp.dot(
            act[...], wout[...], preferred_element_type=jnp.float32
        ).astype(jnp.bfloat16)

    swap_grad.wait_recv()

    def finish_grad(i, carry):
        at = pl.ds(pl.multiple_of(i * step, step), step)
        v = xs[at, :].astype(jnp.float32)
        r = lax.rsqrt(jnp.mean(v * v, axis=-1, keepdims=True) + norm_eps)
        push = (own_terms[0, at, :].astype(jnp.float32) + mp_in[0, at, :].astype(jnp.float32)) * gain
        mixed = jnp.mean(v * push, axis=-1, keepdims=True)
        dx = xc[at, :].astype(jnp.float32) + r * push - v * (r * r * r * mixed)
        z_out[0, at, :] = dx.astype(jnp.bfloat16)
        return carry

    lax.fori_loop(0, rows // step, finish_grad, 0)
    relay_grad = start_remote(z_out.at[0], pass_grad, z_send.at[0], z_recv.at[0], before)

    swap_fwd.wait_recv()
    normalise(xf_peer, nf, rows, rows)
    mp_out[1] = forward(other)
    swap_branch = start_remote(mp_out.at[1], mp_in.at[1], mp_send.at[1], mp_recv.at[1], peer)
    normalise(xf, nf, 0)
    own_terms[1] = forward(own)
    swap_branch.wait_recv()

    def finish_forward(i, carry):
        at = pl.ds(pl.multiple_of(i * step, step), step)
        branch = own_terms[1, at, :].astype(jnp.float32) + mp_in[1, at, :].astype(jnp.float32)
        z_out[1, at, :] = (xf[at, :].astype(jnp.float32) + branch).astype(jnp.bfloat16)
        return carry

    lax.fori_loop(0, rows // step, finish_forward, 0)
    relay_fwd = start_remote(z_out.at[1], pass_fwd, z_send.at[1], z_recv.at[1], after)

    for g in (OUT, IN):
        for h in range(2):
            product(g, h, SECOND)
        for h in range(2):
            sent[g, h, DIAG].wait_recv()
            parts[g, h, SECOND] = (
                parts[g, h, SECOND].astype(jnp.float32) + landed[g, h, DIAG].astype(jnp.float32)
            ).astype(jnp.bfloat16)
            send(g, h, SECOND)
        for h in range(2):
            product(g, h, OWN)
    for g, result in ((OUT, gout_ref), (IN, gin_ref)):
        for h in range(2):
            sent[g, h, DIRECT].wait_recv()
            sent[g, h, SECOND].wait_recv()
            result[halves[h], :] = (
                parts[g, h, OWN].astype(jnp.float32)
                + landed[g, h, DIRECT].astype(jnp.float32)
                + landed[g, h, SECOND].astype(jnp.float32)
            ).astype(jnp.bfloat16)

    relay_grad.wait_recv()
    relay_fwd.wait_recv()
    for copy in [swap_fwd, swap_grad, swap_branch, relay_grad, relay_fwd, *sent.values()]:
        copy.wait_send()


def relay_on_device(fwd_in, stash, cot, w_in, w_out, gain):
    rows, width = stash.shape[1:]
    hid = w_in.shape[1]
    tokens = rows * lax.axis_size("mp")
    cols = width // lax.axis_size("dp")
    half = hid // 2
    bf16 = jnp.bfloat16
    vmem = pl.BlockSpec(memory_space=pltpu.VMEM)
    hbm = pl.BlockSpec(memory_space=pl.ANY)
    dma = pltpu.SemaphoreType.DMA
    held = (tokens * 2 + rows + hid * 2) * width * jnp.dtype(bf16).itemsize
    loaded = pl.pallas_call(
        swap_kernel,
        out_shape=(pltpu.VMEM((tokens, width), bf16),) * 2
        + (pltpu.VMEM((rows, width), bf16),)
        + (pltpu.VMEM((hid, width), bf16),) * 2,
        in_specs=[hbm] * 5,
        out_specs=(vmem,) * 5,
        scratch_shapes=[dma((5,)), dma((2,)), dma((2,))],
        compiler_params=pltpu.CompilerParams(
            collective_id=0, has_side_effects=True,
            vmem_limit_bytes=vmem_bytes - held - 2**17,
        ),
    )(fwd_in[0], stash[0], cot[0], w_in[0], w_out[0])
    results = pl.pallas_call(
        relay_kernel,
        out_shape=(pltpu.VMEM((rows, width), bf16),) * 2 + (pltpu.VMEM((hid, cols), bf16),) * 2,
        in_specs=[vmem] * 6,
        out_specs=(vmem,) * 4,
        scratch_shapes=[
            pltpu.VMEM((rows, width), bf16),
            pltpu.VMEM((tokens, width), bf16),
            pltpu.VMEM((tokens, width), bf16),
            pltpu.VMEM((hid, tokens), jnp.float32),
            pltpu.VMEM((hid, tokens), bf16),
            pltpu.VMEM((hid, tokens), bf16),
            pltpu.VMEM((rows, hid), bf16),
            pltpu.VMEM((2, 2, 4, half, cols), bf16),
            pltpu.VMEM((2, 2, 3, half, cols), bf16),
            pltpu.VMEM((2, rows, width), bf16),
            pltpu.VMEM((2, rows, width), bf16),
            pltpu.VMEM((2, rows, width), bf16),
            pltpu.VMEM((2, rows, width), bf16),
            dma((3,)),
            dma((3,)),
            dma((2, 2, 3)),
            dma((2, 2, 3)),
            dma((2,)),
            dma((2,)),
        ],
        compiler_params=pltpu.CompilerParams(
            collective_id=1, has_side_effects=True, vmem_limit_bytes=40 * 2**20
        ),
    )(*loaded, gain)
    results = pl.pallas_call(
        write_kernel,
        out_shape=tuple(jax.ShapeDtypeStruct(r.shape, r.dtype) for r in results),
        in_specs=[vmem] * 4,
        out_specs=(hbm,) * 4,
        scratch_shapes=[dma((4,))],
        compiler_params=pltpu.CompilerParams(vmem_limit_bytes=4 * 2**20),
    )(*results)
    return tuple(r[None] for r in results)


def fits_relay(mesh):
    return mesh.shape["dp"] == 4 and mesh.shape["mp"] == 2 and mesh.shape["section"] > 1


def solution(mesh):
    in_specs = (
        P("section", ("dp", "mp"), None),
        P("section", ("dp", "mp"), None),
        P("section", ("dp", "mp"), None),
        P("section", "mp", None),
        P("section", "mp", None),
        P("section", None),
    )
    out_specs = (
        P("section", ("dp", "mp"), None),
        P("section", ("dp", "mp"), None),
        P("section", "mp", "dp"),
        P("section", "mp", "dp"),
    )
    return jax.shard_map(
        relay_on_device if fits_relay(mesh) else on_device,
        mesh=mesh,
        in_specs=in_specs,
        out_specs=out_specs,
        check_vma=False,
    )
```
